32 devices in a mesh: gx: 4 (over y, core), gy: 2 (over x), gz: 4 (over z).
Axes of the slice: x: 2, y: 2, z: 4, core: 2. Of those that a mesh axis runs over, the one named last changes fastest.
Arguments:
- positions: float32 [3, 4, 2, 4, 4096], P(None, 'gx', 'gy', 'gz'), may hold values from 0 to 4, as said below
- velocities: float32 [3, 4, 2, 4, 4096], P(None, 'gx', 'gy', 'gz'), may hold values from -6 to 6
- strength: float32 [4, 2, 4, 4096], P('gx', 'gy', 'gz'), may hold values from 0.5 to 2
- charge: float32 [4, 2, 4, 4096], P('gx', 'gy', 'gz'), may hold values from -5 to 5
- bond_stiffness: float32 [2, 4, 2, 4, 4096], P(None, 'gx', 'gy', 'gz'), may hold values from 0.5 to 4
- bond_partner: int32 [2, 4, 2, 4, 4096], P(None, 'gx', 'gy', 'gz'), may hold values from 0 to 18431, as said below
- pair_blocks: int32 [4, 2, 4, 32, 8], P('gx', 'gy', 'gz'), may hold values from 0 to 143, as said below
- tile_count: int32 [4, 2, 4], P('gx', 'gy', 'gz'), may hold values from 1024 to 4096, as said below
- block_cell: int32 [4, 2, 4, 32], P('gx', 'gy', 'gz'), may hold values from 0 to 255
- cell_frac: float32 [3, 256], replicated, may hold values from 0 to 1
- bond_force: float32 [3, 4, 2, 4, 4096], P(None, 'gx', 'gy', 'gz'), may hold values from -6 to 6
- pair_force: float32 [3, 4, 2, 4, 4096], P(None, 'gx', 'gy', 'gz'), may hold values from -6 to 6
- far_force: float32 [3, 4, 2, 4, 4096], P(None, 'gx', 'gy', 'gz'), may hold values from -6 to 6
Outputs:
- positions_out: float32 [3, 4, 2, 4, 4096], P(None, 'gx', 'gy', 'gz')
- velocities_out: float32 [3, 4, 2, 4, 4096], P(None, 'gx', 'gy', 'gz')
The draws below stay inside these ranges and needn't reach their ends.
Inputs may be any that keep to these rules, and one draw needn't show every extreme that they name: `positions`: each bead lies inside the unit cube of its block. `tile_count`: live beads of a tile fill its slots from 0 upward; some tile is full in every draw. `bond_partner`: A live bead's partners are live beads of its own block or of one of the six blocks sharing a face with it; an empty slot names its own column. `pair_blocks`: each row begins with the block itself and then lists distinct blocks that share a face, an edge or a corner with it.
All inputs are finite; a program needn't handle non-finite values.
Results may differ from the reference program's by a relative error of at most 0.0003.
Values sent between devices are 32-bit elements; how exact they have to be, the bound alone decides.
A program may use at most 64 MiB of HBM per device.

```python
import math
import jax
import jax.numpy as jnp
from jax import lax

SBX = 4
SBY = 4
SBZ = 2
BLK = 128
KN = 8
NB = 32
BT = 4096
NTX = 4
NTY = 2
NTZ = 4
CELLS = 256


def block_places():
    block_ids = jnp.arange(SBX * SBY * SBZ, dtype=jnp.int32)
    return (block_ids // (SBY * SBZ), block_ids // SBZ % SBY, block_ids % SBZ)


def extended_block(place_x, place_y, place_z):
    return ((place_x + 1) * (SBY + 2) + place_y + 1) * (SBZ + 2) + place_z + 1


def tile_counts(key):
    base_key = jax.random.fold_in(key, 7001)
    counts = jax.random.randint(base_key, (NTX, NTY, NTZ), BT // 4, BT + 1)
    full_pick = jax.random.randint(jax.random.fold_in(base_key, 1), (3,), 0, 1 << 20)
    counts = counts.at[full_pick[0] % NTX, full_pick[1] % NTY, full_pick[2] % NTZ].set(BT)
    return counts.astype(jnp.int32)


def draw_tile_count(key, part):
    return tile_counts(key)


def draw_positions(key, part):
    inside = jax.random.uniform(jax.random.fold_in(key, 7004), (3, NTX, NTY, NTZ, BT), jnp.float32)
    place_x, place_y, place_z = block_places()
    places = jnp.stack([place_x, place_y, place_z], 0).astype(jnp.float32)
    slot_places = jnp.repeat(places, BLK, axis=1)
    return (inside + slot_places[:, None, None, None, :]).astype(jnp.float32)


def draw_bond_partner(key, part):
    counts = tile_counts(key)
    base_key = jax.random.fold_in(key, 7002)
    block_count = SBX * SBY * SBZ
    full_shape = (2, NTX, NTY, NTZ, block_count, BLK)
    choose_bits = jax.random.randint(jax.random.fold_in(base_key, 1), full_shape, 0, 24)
    face_pick = jnp.where(choose_bits < 18, 0, choose_bits - 17)
    face_moves = ((0, 0, 0), (-1, 0, 0), (1, 0, 0), (0, -1, 0), (0, 1, 0), (0, 0, -1), (0, 0, 1))
    place_x, place_y, place_z = block_places()
    tile_x = jnp.arange(NTX, dtype=jnp.int32)[:, None, None, None]
    tile_y = jnp.arange(NTY, dtype=jnp.int32)[None, :, None, None]
    tile_z = jnp.arange(NTZ, dtype=jnp.int32)[None, None, :, None]
    own_live = jnp.clip(counts[:, :, :, None] - jnp.arange(block_count, dtype=jnp.int32)[None, None, None, :] * BLK, 0, BLK)
    own_ext = extended_block(place_x, place_y, place_z)
    slot_limit = jnp.ones(full_shape, jnp.int32)
    where_block = jnp.zeros(full_shape, jnp.int32)
    for face_index in range(7):
        step_x, step_y, step_z = face_moves[face_index]
        moved_x = place_x + step_x
        moved_y = place_y + step_y
        moved_z = place_z + step_z
        source_x = (tile_x + moved_x[None, None, None, :] // SBX) % NTX
        source_y = (tile_y + moved_y[None, None, None, :] // SBY) % NTY
        source_z = (tile_z + moved_z[None, None, None, :] // SBZ) % NTZ
        source_block = (moved_x % SBX * SBY + moved_y % SBY) * SBZ + moved_z % SBZ
        source_count = counts[source_x, source_y, source_z]
        live_there = jnp.clip(source_count - source_block[None, None, None, :] * BLK, 0, BLK)
        ext_there = extended_block(moved_x, moved_y, moved_z)
        usable = live_there > 0
        limit_here = jnp.where(usable, live_there, own_live)
        ext_here = jnp.where(usable, ext_there[None, None, None, :], own_ext[None, None, None, :])
        chosen = face_pick == face_index
        slot_limit = jnp.where(chosen, limit_here[None, :, :, :, :, None], slot_limit)
        where_block = jnp.where(chosen, ext_here[None, :, :, :, :, None], where_block)
    raw_bits = jax.random.randint(jax.random.fold_in(base_key, 2), full_shape, 0, 1 << 30)
    slot_pick = raw_bits % jnp.maximum(slot_limit, 1)
    partner = (where_block * BLK + slot_pick).reshape(2, NTX, NTY, NTZ, BT)
    slot_ids = jnp.arange(BT, dtype=jnp.int32)
    live_slot = slot_ids[None, None, None, None, :] < counts[None, :, :, :, None]
    itself = jnp.repeat(own_ext, BLK) * BLK + slot_ids % BLK
    return jnp.where(live_slot, partner, itself[None, None, None, None, :]).astype(jnp.int32)


def draw_pair_blocks(key, part):
    block_count = SBX * SBY * SBZ
    base_key = jax.random.fold_in(key, 7003)
    moves = []
    for step_x in (-1, 0, 1):
        for step_y in (-1, 0, 1):
            for step_z in (-1, 0, 1):
                if step_x != 0 or step_y != 0 or step_z != 0:
                    moves.append((step_x, step_y, step_z))
    place_x, place_y, place_z = block_places()
    table = jnp.stack([extended_block(place_x + m[0], place_y + m[1], place_z + m[2]) for m in moves], 1)
    scores = jax.random.randint(base_key, (NTX, NTY, NTZ, block_count, 26), 0, 1 << 30)
    order_ids = jnp.argsort(scores, axis=-1, stable=True)[..., :KN - 1]
    picked = jnp.take_along_axis(jnp.broadcast_to(table, (NTX, NTY, NTZ, block_count, 26)), order_ids, axis=-1)
    own_ext = jnp.broadcast_to(extended_block(place_x, place_y, place_z)[:, None], (NTX, NTY, NTZ, block_count, 1))
    return jnp.concatenate([own_ext, picked], -1).astype(jnp.int32)


def with_ends(values, rng, smallest, high):
    dims = values.shape
    place = [jax.random.randint(jax.random.fold_in(rng, axis), (), 0, dims[axis]) for axis in range(len(dims))]
    values = values.at[tuple(place)].set(smallest)
    longest = dims.index(max(dims))
    place[longest] = (place[longest] + 1) % dims[longest]
    return values.at[tuple(place)].set(high)


def block_levels(rng, dims, cuts, least, largest):
    level, own = 1.0, jax.random.fold_in(rng, 6)
    for position, blocks in cuts:
        steps = jnp.exp(jax.random.uniform(jax.random.fold_in(own, position), (blocks,), jnp.float32, least / len(cuts), largest / len(cuts)))
        level = level * jnp.repeat(steps, dims[position] // blocks).reshape([-1 if axis == position else 1 for axis in range(len(dims))])
    return level


def normal_values(own_key, shape, deviation, most, split=(), kind=jnp.bfloat16):
    loudness = block_levels(own_key, shape, split, -0.22, 0.18) if split else 1.0
    values = jax.random.normal(own_key, shape, jnp.float32) * deviation * loudness
    return jnp.minimum(jnp.maximum(values, -most), most).astype(kind)


def setup_inputs(seed: int = 0) -> dict:
    splits = jax.random.split(jax.random.key(seed), 14)
    return {
        "positions": draw_positions(jax.random.fold_in(splits[13], 71), 0),
        "velocities": normal_values(splits[1], (3, NTX, NTY, NTZ, BT), 1.0, 6.0, ((1, 4), (2, 2), (3, 4)), jnp.float32),
        "strength": jnp.clip(jnp.exp(math.log(2.0) - 1.3862944 * jax.random.uniform(splits[2], (NTX, NTY, NTZ, BT), jnp.float32) ** block_levels(splits[2], (NTX, NTY, NTZ, BT), ((0, 4), (1, 2), (2, 4)), -0.2, 0.2)), 0.5, 2.0),
        "charge": normal_values(splits[3], (NTX, NTY, NTZ, BT), 1.0, 5.0, ((0, 4), (1, 2), (2, 4)), jnp.float32),
        "bond_stiffness": jnp.clip(jnp.exp(math.log(4.0) - 2.0794415 * jax.random.uniform(splits[4], (2, NTX, NTY, NTZ, BT), jnp.float32) ** block_levels(splits[4], (2, NTX, NTY, NTZ, BT), ((1, 4), (2, 2), (3, 4)), -0.2, 0.2)), 0.5, 4.0),
        "bond_partner": draw_bond_partner(jax.random.fold_in(splits[13], 71), 0),
        "pair_blocks": draw_pair_blocks(jax.random.fold_in(splits[13], 71), 0),
        "tile_count": draw_tile_count(jax.random.fold_in(splits[13], 71), 0),
        "block_cell": with_ends(jax.random.randint(splits[8], (NTX, NTY, NTZ, NB), 0, CELLS), jax.random.fold_in(splits[8], 1), 0, CELLS - 1).astype(jnp.int32),
        "cell_frac": jnp.clip(jax.random.uniform(splits[9], (3, CELLS), jnp.float32, 0.0, 1.0), 0.0, 1.0),
        "bond_force": normal_values(splits[10], (3, NTX, NTY, NTZ, BT), 1.0, 6.0, ((1, 4), (2, 2), (3, 4)), jnp.float32),
        "pair_force": normal_values(splits[11], (3, NTX, NTY, NTZ, BT), 1.0, 6.0, ((1, 4), (2, 2), (3, 4)), jnp.float32),
        "far_force": normal_values(splits[12], (3, NTX, NTY, NTZ, BT), 1.0, 6.0, ((1, 4), (2, 2), (3, 4)), jnp.float32),
    }


inner_step = 0.1
gauss_width = 0.25
cutoff_radius = 1.0
pair_scale = 0.1
soften = 1.0
coulomb = 0.02
pair_group = 2

def block_force(own_block, others):
    near_pos = own_block[:3]
    far_pos = others[:3]
    cross_term = jnp.dot(near_pos.T, far_pos, precision=lax.Precision.HIGHEST)
    distance = lax.optimization_barrier(jnp.sum(near_pos * near_pos, 0))[:, None] + lax.optimization_barrier(jnp.sum(far_pos * far_pos, 0))[None, :] - 2.0 * cross_term
    taper_term = jnp.where(distance < cutoff_radius * cutoff_radius, jnp.square(1.0 - distance / (cutoff_radius * cutoff_radius)), 0.0)
    weight = jnp.exp(-distance / (2.0 * gauss_width * gauss_width)) * taper_term * others[3][None, :]
    pulled = jnp.dot(weight, far_pos.T, precision=lax.Precision.HIGHEST)
    weight_sum = lax.optimization_barrier(jnp.sum(weight, 1))
    return pair_scale / (gauss_width * gauss_width) * own_block[3][None, :] * (near_pos * weight_sum[None, :] - pulled.T)

def pair_tile(neighbourhood, blocks, own_packed):
    block_count = blocks.shape[0]
    rows_count = neighbourhood.shape[0]
    grouped = neighbourhood.reshape(rows_count, -1, BLK)
    own_rows = own_packed.reshape(rows_count, block_count, BLK)
    mine_all = jnp.transpose(own_rows, (1, 0, 2)).reshape(block_count // pair_group, pair_group, rows_count, BLK)
    block_lists = blocks.reshape(block_count // pair_group, pair_group, -1)

    def one_block(own_block, chosen):
        others = grouped[:, chosen, :].reshape(rows_count, -1)
        return block_force(own_block, others)

    def one_group(pieces):
        return jax.vmap(one_block)(pieces[0], pieces[1])
    forces = lax.map(one_group, (mine_all, block_lists))
    return jnp.transpose(forces.reshape(block_count, 3, BLK), (1, 0, 2)).reshape(3, -1)

def bond_tile(neighbourhood, partners, stiffness, own_pos):
    result = jnp.zeros_like(own_pos)
    for bond_slot in range(2):
        other_pos = jnp.take(neighbourhood[:3], partners[bond_slot], axis=1)
        result = result - stiffness[bond_slot][None, :] * (own_pos - other_pos)
    return result

def cell_field(totals, centres, targets):
    charge_sum = totals[0]
    dipole = totals[1:4] - charge_sum[None, :] * centres
    separation = targets[:, :, None] - centres[:, None, :]
    inverse = lax.rsqrt(lax.optimization_barrier(jnp.sum(separation * separation, 0)) + soften * soften)
    inverse_cube = inverse * inverse * inverse
    inverse_fifth = inverse_cube * inverse * inverse
    dipole_dot = lax.optimization_barrier(jnp.sum(dipole[:, None, :] * separation, 0))
    field_terms = charge_sum[None, None, :] * separation * inverse_cube - dipole[:, None, :] * inverse_cube + 3.0 * dipole_dot[None] * separation * inverse_fifth
    return lax.optimization_barrier(jnp.sum(field_terms, 2))

def extended_axis(tile_span, sub):
    tiles = jnp.arange(tile_span, dtype=jnp.int32)[:, None]
    cells = jnp.arange(sub + 2, dtype=jnp.int32)[None, :]
    raw = tiles * sub - 1 + cells
    index = (raw % (tile_span * sub)).astype(jnp.int32)
    shift = ((raw // sub - tiles) * sub).astype(jnp.float32)
    return (index, shift)

def neighbourhoods(packed):
    rows_count, size_x, size_y, size_z, bead_count = packed.shape
    grid = packed.reshape(rows_count, size_x, size_y, size_z, SBX, SBY, SBZ, BLK)
    grid = jnp.transpose(grid, (0, 1, 4, 2, 5, 3, 6, 7)).reshape(rows_count, size_x * SBX, size_y * SBY, size_z * SBZ, BLK)
    index_x, shift_x = extended_axis(size_x, SBX)
    index_y, shift_y = extended_axis(size_y, SBY)
    index_z, shift_z = extended_axis(size_z, SBZ)
    grid = jnp.take(grid, index_x.reshape(-1), axis=1)
    grid = jnp.take(grid, index_y.reshape(-1), axis=2)
    grid = jnp.take(grid, index_z.reshape(-1), axis=3)
    grid = grid.reshape(rows_count, size_x, SBX + 2, size_y, SBY + 2, size_z, SBZ + 2, BLK)
    cube_shape = (size_x, SBX + 2, size_y, SBY + 2, size_z, SBZ + 2)
    shift_rows = jnp.stack([jnp.broadcast_to(shift_x[:, :, None, None, None, None], cube_shape), jnp.broadcast_to(shift_y[None, None, :, :, None, None], cube_shape), jnp.broadcast_to(shift_z[None, None, None, None, :, :], cube_shape)], 0)[..., None]
    moved = jnp.concatenate([grid[:3] + shift_rows, grid[3:]], 0)
    moved = jnp.transpose(moved, (1, 3, 5, 0, 2, 4, 6, 7))
    return moved.reshape(size_x * size_y * size_z, rows_count, -1)

def reference(positions, velocities, strength, charge, bond_stiffness, bond_partner, pair_blocks, tile_count, block_cell, cell_frac, bond_force, pair_force, far_force):
    size_x, size_y, size_z, bead_count = strength.shape
    tile_total = size_x * size_y * size_z
    full_shape = positions.shape
    slot_ids = jnp.arange(bead_count, dtype=jnp.int32)
    live_mask = (slot_ids[None, None, None, :] < tile_count[:, :, :, None]).astype(jnp.float32)
    strength_live = strength * live_mask
    charge_live = charge * live_mask
    partners = jnp.transpose(bond_partner.reshape(2, tile_total, bead_count), (1, 0, 2))
    stiffness = jnp.transpose(bond_stiffness.reshape(2, tile_total, bead_count), (1, 0, 2))
    block_lists = pair_blocks.reshape(tile_total, pair_blocks.shape[3], pair_blocks.shape[4])

    def bonds_at(current):
        packed = jnp.concatenate([current, strength_live[None]], 0)
        local_hoods = neighbourhoods(packed)
        own_tiles = jnp.transpose(packed.reshape(4, tile_total, bead_count), (1, 0, 2))

        def one_tile(pieces):
            return bond_tile(pieces[0], pieces[1], pieces[2], pieces[3][:3])
        forces = lax.map(one_tile, (local_hoods, partners, stiffness, own_tiles))
        return (jnp.transpose(forces, (1, 0, 2)).reshape(full_shape), local_hoods, own_tiles)

    def pairs_at(local_hoods, own_tiles):

        def one_tile(pieces):
            return pair_tile(pieces[0], pieces[1], pieces[2])
        forces = lax.map(one_tile, (local_hoods, block_lists, own_tiles))
        return jnp.transpose(forces, (1, 0, 2)).reshape(full_shape)

    def far_at(current):
        corner_x = jnp.broadcast_to(jnp.arange(size_x, dtype=jnp.float32)[:, None, None, None] * SBX, (size_x, size_y, size_z, 1))
        corner_y = jnp.broadcast_to(jnp.arange(size_y, dtype=jnp.float32)[None, :, None, None] * SBY, (size_x, size_y, size_z, 1))
        corner_z = jnp.broadcast_to(jnp.arange(size_z, dtype=jnp.float32)[None, None, :, None] * SBZ, (size_x, size_y, size_z, 1))
        anchor = jnp.stack([corner_x, corner_y, corner_z], 0)
        placed = current + anchor
        block_count = bead_count // BLK
        charge_blocks = charge_live.reshape(size_x, size_y, size_z, block_count, BLK)
        charge_sums = lax.optimization_barrier(jnp.sum(charge_blocks, 4)).reshape(-1)
        weighted = lax.optimization_barrier(jnp.sum((charge_live[None] * placed).reshape(3, size_x, size_y, size_z, block_count, BLK), 5)).reshape(3, -1)
        moments = jnp.concatenate([charge_sums[None], weighted], 0)
        cell_total = cell_frac.shape[1]
        one_hot = (block_cell.reshape(-1)[:, None] == jnp.arange(cell_total, dtype=jnp.int32)[None, :]).astype(jnp.float32)
        totals = jnp.dot(moments, one_hot, precision=lax.Precision.HIGHEST)
        box_size = jnp.array([size_x * SBX, size_y * SBY, size_z * SBZ], dtype=jnp.float32)
        centres = cell_frac * box_size[:, None]
        fields = cell_field(totals, centres, centres)
        block_fields = jnp.dot(fields, one_hot.T, precision=lax.Precision.HIGHEST).reshape(3, size_x, size_y, size_z, block_count)
        return (coulomb * (charge_blocks[None] * block_fields[..., None])).reshape(full_shape)
    half_step = 0.5 * inner_step
    outer_half = 2.0 * inner_step
    current = positions
    velocity_now = velocities + outer_half * far_force + inner_step * pair_force + half_step * bond_force
    bond_now = jnp.zeros_like(current)
    pair_now = jnp.zeros_like(current)
    for inner_index in range(4):
        if inner_index == 2:
            velocity_now = velocity_now + inner_step * pair_now
        if inner_index > 0:
            velocity_now = velocity_now + half_step * bond_now
        current = current + inner_step * velocity_now
        bond_now, local_hoods, own_tiles = bonds_at(current)
        velocity_now = velocity_now + half_step * bond_now
        if inner_index % 2 == 1:
            pair_now = pairs_at(local_hoods, own_tiles)
            velocity_now = velocity_now + inner_step * pair_now
    velocity_now = velocity_now + outer_half * far_at(current)
    return (current, velocity_now)
```

```python
import functools
import itertools
import math

import jax
import jax.numpy as jnp
from jax import lax
from jax.experimental import pallas as pl
from jax.experimental.pallas import tpu as pltpu
from jax.sharding import PartitionSpec as P

SBX = 4
SBY = 4
SBZ = 2
BLK = 128
NB = SBX * SBY * SBZ
AXES = ("gx", "gy", "gz")
SIDES = (SBX, SBY, SBZ)

inner_step = 0.1
outer_half = 2.0 * inner_step
half_step = 0.5 * inner_step
gauss_width = 0.25
cutoff_radius = 1.0
pair_scale = 0.1
soften = 1.0
coulomb = 0.02

MESH = pl.DeviceIdType.MESH
FACES = ((0, 0, 0), (-1, 0, 0), (1, 0, 0), (0, -1, 0), (0, 1, 0), (0, 0, -1), (0, 0, 1))
DIRS = sorted(
    (d for d in itertools.product((-1, 0, 1), repeat=3) if d != (0, 0, 0)),
    key=lambda d: (sum(abs(c) for c in d) != 1, -abs(d[2]), d),
)


def bf(x):
    return x.astype(jnp.bfloat16).astype(jnp.float32)


def split3(x):
    high = bf(x)
    middle = bf(x - high)
    return high, middle, x - high - middle


def kernel(
    sizes,
    pos_ref,
    vel_ref,
    str_ref,
    chg_ref,
    stiff_ref,
    part_ref,
    frac_ref,
    bf_ref,
    pf_ref,
    ff_ref,
    list_ref,
    count_ref,
    cell_ref,
    pos_out,
    vel_out,
    ext,
    v_s,
    spring,
    lane_s,
    face_s,
    own_s,
    far_s,
    val_s,
    hot,
    red_x,
    red_y,
    red_z,
    send_sem,
    recv_sem,
    rsend_sem,
    rrecv_sem,
):
    me = tuple(lax.axis_index(a) for a in AXES)
    cells = frac_ref.shape[1]
    f32 = jnp.float32

    def shifted(axis, step):
        ids = list(me)
        ids[axis] = lax.rem(me[axis] + step + sizes[axis], sizes[axis])
        return tuple(ids)

    def toward(d):
        return tuple(
            me[a] if d[a] == 0 else lax.rem(me[a] + d[a] + sizes[a], sizes[a]) for a in range(3)
        )

    barrier = pltpu.get_barrier_semaphore()
    expected = 0
    for d in DIRS:
        pl.semaphore_signal(barrier, inc=1, device_id=toward(d), device_id_type=MESH)
        expected += 1
    for axis in range(3):
        for step in range(2, sizes[axis] - 1):
            pl.semaphore_signal(barrier, inc=1, device_id=shifted(axis, step), device_id_type=MESH)
            expected += 1

    row4 = lax.broadcasted_iota(jnp.int32, (4, BLK), 0)
    row8 = lax.broadcasted_iota(jnp.int32, (8, BLK), 0)

    def vec4(a, b, c, last=0.0):
        return jnp.where(row4 == 0, a, jnp.where(row4 == 1, b, jnp.where(row4 == 2, c, last)))

    def vec8(a, b, c):
        r = row8 % 4
        return jnp.where(r == 0, a, jnp.where(r == 1, b, jnp.where(r == 2, c, 0.0)))

    coord = row4 < 3

    live = (
        lax.broadcasted_iota(jnp.int32, (NB, BLK), 0) * BLK
        + lax.broadcasted_iota(jnp.int32, (NB, BLK), 1)
        < count_ref[0, 0, 0]
    ).astype(f32)
    strength_live = str_ref[...] * live
    charge_live = chg_ref[...] * live

    def spots(body):
        def plane(bx, carry):
            for by in range(SBY):
                for bz in range(SBZ):
                    body(bx, by, bz, (bx * SBY + by) * SBZ + bz)
            return carry

        lax.fori_loop(0, SBX, plane, 0)

    for bx, by, bz in itertools.product(range(SBX), range(SBY), range(SBZ)):
        b = (bx * SBY + by) * SBZ + bz
        at = (bx, by, bz)
        for c in range(3):
            v = (
                vel_ref[c, b : b + 1, :]
                + outer_half * ff_ref[c, b : b + 1, :]
                + inner_step * pf_ref[c, b : b + 1, :]
                + half_step * bf_ref[c, b : b + 1, :]
            )
            v_s[b, c : c + 1, :] = v
            ext[0, bx + 1, by + 1, bz + 1, c : c + 1, :] = (
                pos_ref[c, b : b + 1, :] - float(at[c])
            ) + inner_step * v
        v_s[b, 3:4, :] = jnp.zeros((1, BLK), f32)
        ext[0, bx + 1, by + 1, bz + 1, 3:4, :] = strength_live[b : b + 1, :]

    pl.semaphore_wait(barrier, expected)

    def box(d, ghost):
        out = []
        for a in range(3):
            if d[a] == 0:
                out.append(pl.ds(1, SIDES[a]))
            elif ghost:
                out.append(pl.ds(0 if d[a] == 1 else SIDES[a] + 1, 1))
            else:
                out.append(pl.ds(SIDES[a] if d[a] == 1 else 1, 1))
        return tuple(out)

    def halo(n, k):
        d = DIRS[k]
        return pltpu.make_async_remote_copy(
            src_ref=ext.at[(n,) + box(d, False)],
            dst_ref=ext.at[(n,) + box(d, True)],
            send_sem=send_sem.at[n, k],
            recv_sem=recv_sem.at[n, k],
            device_id=toward(d),
            device_id_type=MESH,
        )

    reds = (red_x, red_y, red_z)
    base = (0, sizes[0], sizes[0] + sizes[1])

    def exchange(axis, step, slot):
        return pltpu.make_async_remote_copy(
            src_ref=reds[axis].at[slot],
            dst_ref=reds[axis].at[slot],
            send_sem=rsend_sem.at[base[axis] + step],
            recv_sem=rrecv_sem.at[base[axis] + step],
            device_id=shifted(axis, step),
            device_id_type=MESH,
        )

    def reduce_start(axis, value):
        reds[axis][me[axis]] = value
        for step in range(1, sizes[axis]):
            exchange(axis, step, me[axis]).start()

    def reduce_done(axis):
        for step in range(1, sizes[axis]):
            slot = lax.rem(me[axis] - step + sizes[axis], sizes[axis])
            exchange(axis, step, slot).wait_recv()
        total = reds[axis][0]
        for slot in range(1, sizes[axis]):
            total = total + reds[axis][slot]
        return total

    def setup_bonds(bx, by, bz, b):
        blocks, lanes, stiff = [], [], []
        for k in range(2):
            partner = part_ref[k, pl.ds(b, 1), :]
            blocks.append(jnp.broadcast_to(partner // BLK, (4, BLK)))
            lanes.append(jnp.broadcast_to(partner % BLK, (4, BLK)))
            stiff.append(jnp.where(coord, stiff_ref[k, pl.ds(b, 1), :], 0.0))
        block = jnp.concatenate(blocks, 0)
        lane_s[b] = jnp.concatenate(lanes, 0)
        spring[b] = jnp.concatenate(stiff, 0)
        face = jnp.zeros((8, BLK), jnp.int32)
        for f in range(1, 7):
            m = FACES[f]
            place = ((bx + 1 + m[0]) * (SBY + 2) + by + 1 + m[1]) * (SBZ + 2) + bz + 1 + m[2]
            face = jnp.where(block == place, f, face)
        face_s[b] = face

    def bond(n, bx, by, bz, b):
        own = ext[n, bx + 1, by + 1, bz + 1]
        lanes = lane_s[b]
        face = face_s[b]
        got = None
        for f in range(7):
            m = FACES[f]
            source = own if f == 0 else ext[n, bx + 1 + m[0], by + 1 + m[1], bz + 1 + m[2]]
            twice = jnp.concatenate([source, source], 0)
            found = jnp.take_along_axis(twice, lanes, axis=1, mode="promise_in_bounds")
            if f == 0:
                got = found
            else:
                got = jnp.where(face == f, found + vec8(*(float(c) for c in m)), got)
        pull = spring[b] * (got - jnp.concatenate([own, own], 0))
        return own, pull[:4] + pull[4:]

    def prepare(n, ex, ey, ez, mine=None):
        block = ext[n, ex, ey, ez]
        off = vec4(
            jnp.asarray(ex - 1, f32), jnp.asarray(ey - 1, f32), jnp.asarray(ez - 1, f32)
        )
        x = block + off
        square = jnp.where(coord, x * x, 0.0)
        norm = jnp.sum(square, 0, keepdims=True)
        amount = block[3:4]
        first = jnp.where(row4 == 0, 1.0, 0.0)
        other = jnp.concatenate([jnp.where(coord, -2.0 * x, norm), first], 0)
        h, m, l = split3(other)
        e = (ex * (SBY + 2) + ey) * (SBZ + 2) + ez
        far_s[e] = jnp.concatenate([h, m, h, m, l, h], 0).astype(jnp.bfloat16)
        vh, vm, vl = split3(jnp.where(coord, x * amount, amount))
        val_s[e] = jnp.concatenate([vh, vm, vl, jnp.zeros((4, BLK), f32)], 0).astype(jnp.bfloat16)
        if mine is not None:
            own = jnp.concatenate(
                [jnp.where(coord, x, 1.0), jnp.where(row4 == 0, norm, 0.0)], 0
            )
            h, m, l = split3(own)
            stack = jnp.concatenate([h, h, m, m, h, l, jnp.zeros((80, BLK), f32)], 0)
            own_s[mine] = jnp.transpose(stack)[:, :48].astype(jnp.bfloat16)

    def prepare_ghosts(n):
        def side_x(i, carry):
            for ez in range(SBZ + 2):
                prepare(n, 0, i, ez)
                prepare(n, SBX + 1, i, ez)
            return carry

        lax.fori_loop(0, SBY + 2, side_x, 0)

        def side_yz(i, carry):
            for ez in range(SBZ + 2):
                prepare(n, i, 0, ez)
                prepare(n, i, SBY + 1, ez)
            for ey in range(1, SBY + 1):
                prepare(n, i, ey, 0)
                prepare(n, i, ey, SBZ + 1)
            return carry

        lax.fori_loop(1, SBX + 1, side_yz, 0)

    scale = -math.log2(math.e) / (2.0 * gauss_width * gauss_width)

    def pair(n, bx, by, bz, b):
        own = own_s[b]
        acc = jnp.zeros((BLK, 16), f32)
        for j in range(0, list_ref.shape[1], 2):
            p, q = list_ref[b, j], list_ref[b, j + 1]
            far = jnp.concatenate([far_s[p], far_s[q]], 1)
            val = jnp.concatenate([val_s[p], val_s[q]], 1)
            distance = lax.dot_general(
                own, far, (((1,), (0,)), ((), ())), preferred_element_type=f32
            )
            taper = jnp.maximum(1.0 - distance * (1.0 / (cutoff_radius * cutoff_radius)), 0.0)
            weight = jnp.exp2(distance * scale) * (taper * taper)
            high = weight.astype(jnp.bfloat16)
            low = (weight - high.astype(f32)).astype(jnp.bfloat16)
            for part in (high, low):
                acc = acc + lax.dot_general(
                    part, val, (((1,), (1,)), ((), ())), preferred_element_type=f32
                )
        sums = jnp.transpose(acc)
        sums = sums[0:4] + sums[4:8] + sums[8:12]
        block = ext[n, bx + 1, by + 1, bz + 1]
        x = block + vec4(jnp.asarray(bx, f32), jnp.asarray(by, f32), jnp.asarray(bz, f32))
        force = block[3:4] * (x * sums[3:4] - sums)
        return jnp.where(coord, (pair_scale / (gauss_width * gauss_width)) * force, 0.0)

    def start_halo(n):
        for k in range(26 if n % 2 else 6):
            halo(n, k).start()

    def wait_halo(n, lo, hi):
        for k in range(lo, hi):
            halo(n, k).wait_recv()

    def bond_step(n, kick, drift):
        def body(bx, by, bz, b):
            own, force = bond(n, bx, by, bz, b)
            v = v_s[b] + kick * force
            v_s[b] = v
            if drift:
                ext[n + 1, bx + 1, by + 1, bz + 1] = own + inner_step * v

        spots(body)

    start_halo(0)
    spots(setup_bonds)
    wait_halo(0, 0, 6)
    bond_step(0, inner_step, True)

    start_halo(1)
    spots(lambda bx, by, bz, b: prepare(1, bx + 1, by + 1, bz + 1, b))
    wait_halo(1, 0, 26)
    bond_step(1, inner_step, False)
    prepare_ghosts(1)

    def middle(b, carry):
        bx, by, bz = b // (SBY * SBZ), b // SBZ % SBY, b % SBZ
        v = v_s[b] + (2.0 * inner_step) * pair(1, bx, by, bz, b)
        v_s[b] = v
        ext[2, bx + 1, by + 1, bz + 1] = ext[1, bx + 1, by + 1, bz + 1] + inner_step * v
        return carry

    lax.fori_loop(0, NB, middle, 0)

    start_halo(2)
    cell_ids = lax.broadcasted_iota(jnp.int32, (1, cells), 1)
    for b in range(NB):
        hot[b : b + 1, :] = jnp.where(cell_ids == cell_ref[0, 0, 0, b], 1.0, 0.0)
    wait_halo(2, 0, 6)
    bond_step(2, inner_step, True)

    start_halo(3)
    moments = jnp.zeros((4, cells), f32)
    for bx, by, bz in itertools.product(range(SBX), range(SBY), range(SBZ)):
        b = (bx * SBY + by) * SBZ + bz
        block = ext[3, bx + 1, by + 1, bz + 1]
        placed = jnp.where(
            coord,
            block
            + vec4(
                (me[0] * SBX + bx).astype(f32),
                (me[1] * SBY + by).astype(f32),
                (me[2] * SBZ + bz).astype(f32),
            ),
            1.0,
        )
        summed = jnp.sum(placed * charge_live[b : b + 1, :], 1, keepdims=True)
        moments = moments + summed * hot[b : b + 1, :]
        for c in range(3):
            pos_out[c, b : b + 1, :] = block[c : c + 1] + float((bx, by, bz)[c])
    reduce_start(0, moments)
    spots(lambda bx, by, bz, b: prepare(3, bx + 1, by + 1, bz + 1, b))
    wait_halo(3, 0, 26)
    bond_step(3, half_step, False)
    prepare_ghosts(3)

    def final(b, carry):
        bx, by, bz = b // (SBY * SBZ), b // SBZ % SBY, b % SBZ
        v_s[b] = v_s[b] + inner_step * pair(3, bx, by, bz, b)
        return carry

    quarter = NB // 4
    lax.fori_loop(0, quarter, final, 0)
    reduce_start(1, reduce_done(0))
    lax.fori_loop(quarter, 2 * quarter, final, 0)
    reduce_start(2, reduce_done(1))
    lax.fori_loop(2 * quarter, NB, final, 0)
    totals = reduce_done(2)

    one_hot = hot[...]
    charge_sum = totals[3:4]
    separation, dipole, centres = [], [], []
    for c in range(3):
        centre = frac_ref[c : c + 1, :] * float(sizes[c] * SIDES[c])
        target = jnp.sum(one_hot * centre, 1, keepdims=True)
        separation.append(target - centre)
        dipole.append(totals[c : c + 1] - charge_sum * centre)
    distance = sum(s * s for s in separation) + soften * soften
    inverse = lax.rsqrt(distance)
    cube = inverse * inverse * inverse
    fifth = cube * inverse * inverse
    dot = sum(d * s for d, s in zip(dipole, separation))
    along = charge_sum * cube + 3.0 * dot * fifth
    for b in range(NB):
        for c in range(3):
            vel_out[c, b : b + 1, :] = v_s[b, c : c + 1, :]
    for c in range(3):
        field = jnp.sum(along * separation[c] - dipole[c] * cube, 1, keepdims=True)
        vel_out[c] = vel_out[c] + outer_half * coulomb * (charge_live * field)

    for n in range(4):
        for k in range(26 if n % 2 else 6):
            halo(n, k).wait_send()
    for axis in range(3):
        for step in range(1, sizes[axis]):
            exchange(axis, step, me[axis]).wait_send()


def per_device(
    sizes,
    positions,
    velocities,
    strength,
    charge,
    bond_stiffness,
    bond_partner,
    pair_blocks,
    tile_count,
    block_cell,
    cell_frac,
    bond_force,
    pair_force,
    far_force,
):
    f32 = jnp.float32
    cells = cell_frac.shape[1]
    vmem = pl.BlockSpec(memory_space=pltpu.VMEM)
    smem = pl.BlockSpec(memory_space=pltpu.SMEM)
    wide = lambda x: x.reshape(x.shape[0], NB, BLK)
    flat = lambda x: x.reshape(NB, BLK)
    moved = sum(sizes)
    outs = pl.pallas_call(
        functools.partial(kernel, sizes),
        out_shape=[jax.ShapeDtypeStruct((3, NB, BLK), f32)] * 2,
        in_specs=[vmem] * 10 + [smem] * 3,
        out_specs=[vmem] * 2,
        scratch_shapes=[
            pltpu.VMEM((4, SBX + 2, SBY + 2, SBZ + 2, 4, BLK), f32),
            pltpu.VMEM((NB, 4, BLK), f32),
            pltpu.VMEM((NB, 8, BLK), f32),
            pltpu.VMEM((NB, 8, BLK), jnp.int32),
            pltpu.VMEM((NB, 8, BLK), jnp.int32),
            pltpu.VMEM((NB, BLK, 48), jnp.bfloat16),
            pltpu.VMEM(((SBX + 2) * (SBY + 2) * (SBZ + 2), 48, BLK), jnp.bfloat16),
            pltpu.VMEM(((SBX + 2) * (SBY + 2) * (SBZ + 2), 16, BLK), jnp.bfloat16),
            pltpu.VMEM((NB, cells), f32),
            pltpu.VMEM((sizes[0], 4, cells), f32),
            pltpu.VMEM((sizes[1], 4, cells), f32),
            pltpu.VMEM((sizes[2], 4, cells), f32),
            pltpu.SemaphoreType.DMA((4, 26)),
            pltpu.SemaphoreType.DMA((4, 26)),
            pltpu.SemaphoreType.DMA((moved,)),
            pltpu.SemaphoreType.DMA((moved,)),
        ],
        compiler_params=pltpu.CompilerParams(collective_id=0, has_side_effects=True),
    )(
        wide(positions),
        wide(velocities),
        flat(strength),
        flat(charge),
        wide(bond_stiffness),
        wide(bond_partner),
        cell_frac,
        wide(bond_force),
        wide(pair_force),
        wide(far_force),
        pair_blocks.reshape(pair_blocks.shape[3:]),
        tile_count,
        block_cell,
    )
    return outs[0].reshape(positions.shape), outs[1].reshape(velocities.shape)


def solution(mesh):
    sizes = tuple(mesh.shape[a] for a in AXES)
    in_specs = (
        P(None, "gx", "gy", "gz", None),
        P(None, "gx", "gy", "gz", None),
        P("gx", "gy", "gz", None),
        P("gx", "gy", "gz", None),
        P(None, "gx", "gy", "gz", None),
        P(None, "gx", "gy", "gz", None),
        P("gx", "gy", "gz", None, None),
        P("gx", "gy", "gz"),
        P("gx", "gy", "gz", None),
        P(),
        P(None, "gx", "gy", "gz", None),
        P(None, "gx", "gy", "gz", None),
        P(None, "gx", "gy", "gz", None),
    )
    out_specs = (P(None, "gx", "gy", "gz", None), P(None, "gx", "gy", "gz", None))
    return jax.shard_map(
        functools.partial(per_device, sizes),
        mesh=mesh,
        in_specs=in_specs,
        out_specs=out_specs,
        check_vma=False,
    )
```

```python
import functools
import itertools
import math

import jax
import jax.numpy as jnp
from jax import lax
from jax.experimental import pallas as pl
from jax.experimental.pallas import tpu as pltpu
from jax.sharding import PartitionSpec as P

SBX = 4
SBY = 4
SBZ = 2
BLK = 128
NB = SBX * SBY * SBZ
AXES = ("gx", "gy", "gz")
SIDES = (SBX, SBY, SBZ)

inner_step = 0.1
outer_half = 2.0 * inner_step
half_step = 0.5 * inner_step
gauss_width = 0.25
cutoff_radius = 1.0
pair_scale = 0.1
soften = 1.0
coulomb = 0.02

MESH = pl.DeviceIdType.MESH
FACES = ((0, 0, 0), (-1, 0, 0), (1, 0, 0), (0, -1, 0), (0, 1, 0), (0, 0, -1), (0, 0, 1))
DIRS = sorted(
    (d for d in itertools.product((-1, 0, 1), repeat=3) if d != (0, 0, 0)),
    key=lambda d: (sum(abs(c) for c in d) != 1, -abs(d[2]), d),
)


def bf(x):
    return x.astype(jnp.bfloat16).astype(jnp.float32)


def split3(x):
    high = bf(x)
    middle = bf(x - high)
    return high, middle, x - high - middle


def kernel(sizes, *refs):
    fetched, sem = refs[-11:-1], refs[-1]
    copies = [pltpu.make_async_copy(refs[i], fetched[i], sem.at[i]) for i in range(10)]
    for copy in copies:
        copy.start()
    body(sizes, copies, *fetched, *refs[10:-11])


def body(
    sizes,
    copies,
    pos_ref,
    vel_ref,
    str_ref,
    chg_ref,
    stiff_ref,
    part_ref,
    frac_ref,
    bf_ref,
    pf_ref,
    ff_ref,
    list_ref,
    count_ref,
    cell_ref,
    pos_out,
    vel_out,
    ext,
    v_s,
    spring,
    lane_s,
    face_s,
    own_s,
    far_s,
    val_s,
    hot,
    red_x,
    red_y,
    red_z,
    send_sem,
    recv_sem,
    rsend_sem,
    rrecv_sem,
):
    me = tuple(lax.axis_index(a) for a in AXES)
    cells = frac_ref.shape[1]
    f32 = jnp.float32

    def shifted(axis, step):
        ids = list(me)
        ids[axis] = lax.rem(me[axis] + step + sizes[axis], sizes[axis])
        return tuple(ids)

    def toward(d):
        return tuple(
            me[a] if d[a] == 0 else lax.rem(me[a] + d[a] + sizes[a], sizes[a]) for a in range(3)
        )

    barrier = pltpu.get_barrier_semaphore()
    expected = 0
    for d in DIRS:
        pl.semaphore_signal(barrier, inc=1, device_id=toward(d), device_id_type=MESH)
        expected += 1
    for axis in range(3):
        for step in range(2, sizes[axis] - 1):
            pl.semaphore_signal(barrier, inc=1, device_id=shifted(axis, step), device_id_type=MESH)
            expected += 1

    for copy in copies:
        copy.wait()

    row4 = lax.broadcasted_iota(jnp.int32, (4, BLK), 0)
    row8 = lax.broadcasted_iota(jnp.int32, (8, BLK), 0)

    def vec4(a, b, c, last=0.0):
        return jnp.where(row4 == 0, a, jnp.where(row4 == 1, b, jnp.where(row4 == 2, c, last)))

    def vec8(a, b, c):
        r = row8 % 4
        return jnp.where(r == 0, a, jnp.where(r == 1, b, jnp.where(r == 2, c, 0.0)))

    coord = row4 < 3

    live = (
        lax.broadcasted_iota(jnp.int32, (NB, BLK), 0) * BLK
        + lax.broadcasted_iota(jnp.int32, (NB, BLK), 1)
        < count_ref[0, 0, 0]
    ).astype(f32)
    strength_live = str_ref[...] * live
    charge_live = chg_ref[...] * live

    def spots(body):
        def plane(bx, carry):
            for by in range(SBY):
                for bz in range(SBZ):
                    body(bx, by, bz, (bx * SBY + by) * SBZ + bz)
            return carry

        lax.fori_loop(0, SBX, plane, 0)

    for bx, by, bz in itertools.product(range(SBX), range(SBY), range(SBZ)):
        b = (bx * SBY + by) * SBZ + bz
        at = (bx, by, bz)
        for c in range(3):
            v = (
                vel_ref[c, b : b + 1, :]
                + outer_half * ff_ref[c, b : b + 1, :]
                + inner_step * pf_ref[c, b : b + 1, :]
                + half_step * bf_ref[c, b : b + 1, :]
            )
            v_s[b, c : c + 1, :] = v
            ext[0, bx + 1, by + 1, bz + 1, c : c + 1, :] = (
                pos_ref[c, b : b + 1, :] - float(at[c])
            ) + inner_step * v
        v_s[b, 3:4, :] = jnp.zeros((1, BLK), f32)
        ext[0, bx + 1, by + 1, bz + 1, 3:4, :] = strength_live[b : b + 1, :]

    pl.semaphore_wait(barrier, expected)

    def box(d, ghost):
        out = []
        for a in range(3):
            if d[a] == 0:
                out.append(pl.ds(1, SIDES[a]))
            elif ghost:
                out.append(pl.ds(0 if d[a] == 1 else SIDES[a] + 1, 1))
            else:
                out.append(pl.ds(SIDES[a] if d[a] == 1 else 1, 1))
        return tuple(out)

    def halo(n, k):
        d = DIRS[k]
        return pltpu.make_async_remote_copy(
            src_ref=ext.at[(n,) + box(d, False)],
            dst_ref=ext.at[(n,) + box(d, True)],
            send_sem=send_sem.at[n, k],
            recv_sem=recv_sem.at[n, k],
            device_id=toward(d),
            device_id_type=MESH,
        )

    reds = (red_x, red_y, red_z)
    base = (0, sizes[0], sizes[0] + sizes[1])

    def exchange(axis, step, slot):
        return pltpu.make_async_remote_copy(
            src_ref=reds[axis].at[slot],
            dst_ref=reds[axis].at[slot],
            send_sem=rsend_sem.at[base[axis] + step],
            recv_sem=rrecv_sem.at[base[axis] + step],
            device_id=shifted(axis, step),
            device_id_type=MESH,
        )

    def reduce_start(axis, value):
        reds[axis][me[axis]] = value
        for step in range(1, sizes[axis]):
            exchange(axis, step, me[axis]).start()

    def reduce_done(axis):
        for step in range(1, sizes[axis]):
            slot = lax.rem(me[axis] - step + sizes[axis], sizes[axis])
            exchange(axis, step, slot).wait_recv()
        total = reds[axis][0]
        for slot in range(1, sizes[axis]):
            total = total + reds[axis][slot]
        return total

    def setup_bonds(bx, by, bz, b):
        blocks, lanes, stiff = [], [], []
        for k in range(2):
            partner = part_ref[k, pl.ds(b, 1), :]
            blocks.append(jnp.broadcast_to(partner // BLK, (4, BLK)))
            lanes.append(jnp.broadcast_to(partner % BLK, (4, BLK)))
            stiff.append(jnp.where(coord, stiff_ref[k, pl.ds(b, 1), :], 0.0))
        block = jnp.concatenate(blocks, 0)
        lane_s[b] = jnp.concatenate(lanes, 0)
        spring[b] = jnp.concatenate(stiff, 0)
        face = jnp.zeros((8, BLK), jnp.int32)
        for f in range(1, 7):
            m = FACES[f]
            place = ((bx + 1 + m[0]) * (SBY + 2) + by + 1 + m[1]) * (SBZ + 2) + bz + 1 + m[2]
            face = jnp.where(block == place, f, face)
        face_s[b] = face

    def bond(n, bx, by, bz, b):
        own = ext[n, bx + 1, by + 1, bz + 1]
        lanes = lane_s[b]
        face = face_s[b]
        got = None
        for f in range(7):
            m = FACES[f]
            source = own if f == 0 else ext[n, bx + 1 + m[0], by + 1 + m[1], bz + 1 + m[2]]
            twice = jnp.concatenate([source, source], 0)
            found = jnp.take_along_axis(twice, lanes, axis=1, mode="promise_in_bounds")
            if f == 0:
                got = found
            else:
                got = jnp.where(face == f, found + vec8(*(float(c) for c in m)), got)
        pull = spring[b] * (got - jnp.concatenate([own, own], 0))
        return own, pull[:4] + pull[4:]

    def prepare(n, ex, ey, ez, mine=None):
        block = ext[n, ex, ey, ez]
        off = vec4(
            jnp.asarray(ex - 1, f32), jnp.asarray(ey - 1, f32), jnp.asarray(ez - 1, f32)
        )
        x = block + off
        square = jnp.where(coord, x * x, 0.0)
        norm = jnp.sum(square, 0, keepdims=True)
        amount = block[3:4]
        first = jnp.where(row4 == 0, 1.0, 0.0)
        other = jnp.concatenate([jnp.where(coord, -2.0 * x, norm), first], 0)
        h, m, l = split3(other)
        e = (ex * (SBY + 2) + ey) * (SBZ + 2) + ez
        far_s[e] = jnp.concatenate([h, m, h, m, l, h], 0).astype(jnp.bfloat16)
        vh, vm, vl = split3(jnp.where(coord, x * amount, amount))
        val_s[e] = jnp.concatenate([vh, vm, vl, jnp.zeros((4, BLK), f32)], 0).astype(jnp.bfloat16)
        if mine is not None:
            own = jnp.concatenate(
                [jnp.where(coord, x, 1.0), jnp.where(row4 == 0, norm, 0.0)], 0
            )
            h, m, l = split3(own)
            stack = jnp.concatenate([h, h, m, m, h, l, jnp.zeros((80, BLK), f32)], 0)
            own_s[mine] = jnp.transpose(stack)[:, :48].astype(jnp.bfloat16)

    def prepare_ghosts(n):
        def side_x(i, carry):
            for ez in range(SBZ + 2):
                prepare(n, 0, i, ez)
                prepare(n, SBX + 1, i, ez)
            return carry

        lax.fori_loop(0, SBY + 2, side_x, 0)

        def side_yz(i, carry):
            for ez in range(SBZ + 2):
                prepare(n, i, 0, ez)
                prepare(n, i, SBY + 1, ez)
            for ey in range(1, SBY + 1):
                prepare(n, i, ey, 0)
                prepare(n, i, ey, SBZ + 1)
            return carry

        lax.fori_loop(1, SBX + 1, side_yz, 0)

    scale = -math.log2(math.e) / (2.0 * gauss_width * gauss_width)

    def pair(n, bx, by, bz, b):
        own = own_s[b]
        highs, lows, vals = [], [], []
        for j in range(0, list_ref.shape[0], 2):
            p, q = list_ref[j, b], list_ref[j + 1, b]
            far = jnp.concatenate([far_s[p], far_s[q]], 1)
            vals.append(jnp.concatenate([val_s[p], val_s[q]], 1))
            distance = lax.dot_general(
                own, far, (((1,), (0,)), ((), ())), preferred_element_type=f32
            )
            taper = jnp.maximum(1.0 - distance * (1.0 / (cutoff_radius * cutoff_radius)), 0.0)
            weight = jnp.exp2(distance * scale) * (taper * taper)
            high = weight.astype(jnp.bfloat16)
            highs.append(high)
            lows.append((weight - high.astype(f32)).astype(jnp.bfloat16))
        acc = lax.dot_general(
            jnp.concatenate(highs + lows, 1), jnp.concatenate(vals + vals, 1),
            (((1,), (1,)), ((), ())), preferred_element_type=f32,
        )
        sums = jnp.transpose(acc)
        sums = sums[0:4] + sums[4:8] + sums[8:12]
        block = ext[n, bx + 1, by + 1, bz + 1]
        x = block + vec4(jnp.asarray(bx, f32), jnp.asarray(by, f32), jnp.asarray(bz, f32))
        force = block[3:4] * (x * sums[3:4] - sums)
        return jnp.where(coord, (pair_scale / (gauss_width * gauss_width)) * force, 0.0)

    def start_halo(n):
        for k in range(26 if n % 2 else 6):
            halo(n, k).start()

    def wait_halo(n, lo, hi):
        for k in range(lo, hi):
            halo(n, k).wait_recv()

    def bond_step(n, kick, drift):
        def body(bx, by, bz, b):
            own, force = bond(n, bx, by, bz, b)
            v = v_s[b] + kick * force
            v_s[b] = v
            if drift:
                ext[n + 1, bx + 1, by + 1, bz + 1] = own + inner_step * v

        spots(body)

    start_halo(0)
    spots(setup_bonds)
    wait_halo(0, 0, 6)
    bond_step(0, inner_step, True)

    start_halo(1)
    spots(lambda bx, by, bz, b: prepare(1, bx + 1, by + 1, bz + 1, b))
    wait_halo(1, 0, 6)
    bond_step(1, inner_step, False)
    wait_halo(1, 6, 26)
    prepare_ghosts(1)

    def middle(b, carry):
        bx, by, bz = b // (SBY * SBZ), b // SBZ % SBY, b % SBZ
        v = v_s[b] + (2.0 * inner_step) * pair(1, bx, by, bz, b)
        v_s[b] = v
        ext[2, bx + 1, by + 1, bz + 1] = ext[1, bx + 1, by + 1, bz + 1] + inner_step * v
        return carry

    lax.fori_loop(0, NB, middle, 0, unroll=4)

    start_halo(2)
    cell_ids = lax.broadcasted_iota(jnp.int32, (1, cells), 1)
    for b in range(NB):
        hot[b : b + 1, :] = jnp.where(cell_ids == cell_ref[0, 0, 0, b], 1.0, 0.0)
    wait_halo(2, 0, 6)
    bond_step(2, inner_step, True)

    start_halo(3)
    moments = jnp.zeros((4, cells), f32)
    for bx, by, bz in itertools.product(range(SBX), range(SBY), range(SBZ)):
        b = (bx * SBY + by) * SBZ + bz
        block = ext[3, bx + 1, by + 1, bz + 1]
        placed = jnp.where(
            coord,
            block
            + vec4(
                (me[0] * SBX + bx).astype(f32),
                (me[1] * SBY + by).astype(f32),
                (me[2] * SBZ + bz).astype(f32),
            ),
            1.0,
        )
        summed = jnp.sum(placed * charge_live[b : b + 1, :], 1, keepdims=True)
        moments = moments + summed * hot[b : b + 1, :]
        for c in range(3):
            pos_out[c, b : b + 1, :] = block[c : c + 1] + float((bx, by, bz)[c])
    reduce_start(0, moments)
    spots(lambda bx, by, bz, b: prepare(3, bx + 1, by + 1, bz + 1, b))
    wait_halo(3, 0, 6)
    bond_step(3, half_step, False)
    wait_halo(3, 6, 26)
    prepare_ghosts(3)

    def final(b, carry):
        bx, by, bz = b // (SBY * SBZ), b // SBZ % SBY, b % SBZ
        v_s[b] = v_s[b] + inner_step * pair(3, bx, by, bz, b)
        return carry

    quarter = NB // 4
    lax.fori_loop(0, quarter, final, 0, unroll=4)
    reduce_start(1, reduce_done(0))
    lax.fori_loop(quarter, 2 * quarter, final, 0, unroll=4)
    reduce_start(2, reduce_done(1))
    lax.fori_loop(2 * quarter, NB, final, 0, unroll=4)
    totals = reduce_done(2)

    one_hot = hot[...]
    charge_sum = totals[3:4]
    separation, dipole, centres = [], [], []
    for c in range(3):
        centre = frac_ref[c : c + 1, :] * float(sizes[c] * SIDES[c])
        target = jnp.sum(one_hot * centre, 1, keepdims=True)
        separation.append(target - centre)
        dipole.append(totals[c : c + 1] - charge_sum * centre)
    distance = sum(s * s for s in separation) + soften * soften
    inverse = lax.rsqrt(distance)
    cube = inverse * inverse * inverse
    fifth = cube * inverse * inverse
    dot = sum(d * s for d, s in zip(dipole, separation))
    along = charge_sum * cube + 3.0 * dot * fifth
    for b in range(NB):
        for c in range(3):
            vel_out[c, b : b + 1, :] = v_s[b, c : c + 1, :]
    for c in range(3):
        field = jnp.sum(along * separation[c] - dipole[c] * cube, 1, keepdims=True)
        vel_out[c] = vel_out[c] + outer_half * coulomb * (charge_live * field)

    for n in range(4):
        for k in range(26 if n % 2 else 6):
            halo(n, k).wait_send()
    for axis in range(3):
        for step in range(1, sizes[axis]):
            exchange(axis, step, me[axis]).wait_send()


def per_device(
    sizes,
    positions,
    velocities,
    strength,
    charge,
    bond_stiffness,
    bond_partner,
    pair_blocks,
    tile_count,
    block_cell,
    cell_frac,
    bond_force,
    pair_force,
    far_force,
):
    f32 = jnp.float32
    cells = cell_frac.shape[1]
    vmem = pl.BlockSpec(memory_space=pltpu.VMEM)
    smem = pl.BlockSpec(memory_space=pltpu.SMEM)
    wide = lambda x: x.reshape(x.shape[0], NB, BLK)
    flat = lambda x: x.reshape(NB, BLK)
    moved = sum(sizes)
    operands = (
        wide(positions),
        wide(velocities),
        flat(strength),
        flat(charge),
        wide(bond_stiffness),
        wide(bond_partner),
        cell_frac,
        wide(bond_force),
        wide(pair_force),
        wide(far_force),
    )
    outs = pl.pallas_call(
        functools.partial(kernel, sizes),
        out_shape=[jax.ShapeDtypeStruct((3, NB, BLK), f32)] * 2,
        in_specs=[pl.BlockSpec(memory_space=pl.ANY)] * 10 + [smem] * 3,
        out_specs=[vmem] * 2,
        scratch_shapes=[
            pltpu.VMEM((4, SBX + 2, SBY + 2, SBZ + 2, 4, BLK), f32),
            pltpu.VMEM((NB, 4, BLK), f32),
            pltpu.VMEM((NB, 8, BLK), f32),
            pltpu.VMEM((NB, 8, BLK), jnp.int32),
            pltpu.VMEM((NB, 8, BLK), jnp.int32),
            pltpu.VMEM((NB, BLK, 48), jnp.bfloat16),
            pltpu.VMEM(((SBX + 2) * (SBY + 2) * (SBZ + 2), 48, BLK), jnp.bfloat16),
            pltpu.VMEM(((SBX + 2) * (SBY + 2) * (SBZ + 2), 16, BLK), jnp.bfloat16),
            pltpu.VMEM((NB, cells), f32),
            pltpu.VMEM((sizes[0], 4, cells), f32),
            pltpu.VMEM((sizes[1], 4, cells), f32),
            pltpu.VMEM((sizes[2], 4, cells), f32),
            pltpu.SemaphoreType.DMA((4, 26)),
            pltpu.SemaphoreType.DMA((4, 26)),
            pltpu.SemaphoreType.DMA((moved,)),
            pltpu.SemaphoreType.DMA((moved,)),
            *[pltpu.VMEM(x.shape, x.dtype) for x in operands],
            pltpu.SemaphoreType.DMA((len(operands),)),
        ],
        compiler_params=pltpu.CompilerParams(collective_id=0, has_side_effects=True),
    )(
        *operands,
        jnp.swapaxes(pair_blocks.reshape(pair_blocks.shape[3:]), 0, 1),
        tile_count,
        block_cell,
    )
    return outs[0].reshape(positions.shape), outs[1].reshape(velocities.shape)


def solution(mesh):
    sizes = tuple(mesh.shape[a] for a in AXES)
    in_specs = (
        P(None, "gx", "gy", "gz", None),
        P(None, "gx", "gy", "gz", None),
        P("gx", "gy", "gz", None),
        P("gx", "gy", "gz", None),
        P(None, "gx", "gy", "gz", None),
        P(None, "gx", "gy", "gz", None),
        P("gx", "gy", "gz", None, None),
        P("gx", "gy", "gz"),
        P("gx", "gy", "gz", None),
        P(),
        P(None, "gx", "gy", "gz", None),
        P(None, "gx", "gy", "gz", None),
        P(None, "gx", "gy", "gz", None),
    )
    out_specs = (P(None, "gx", "gy", "gz", None), P(None, "gx", "gy", "gz", None))
    return jax.shard_map(
        functools.partial(per_device, sizes),
        mesh=mesh,
        in_specs=in_specs,
        out_specs=out_specs,
        check_vma=False,
    )
```
